256 devices in a mesh: ep: 16 (over y, z_lo, core), etp: 16 (over z_hi, x).
Axes of the slice: x: 4, y: 4, z: 8 (z_hi: 4, z_lo: 2; z = z_hi * 2 + z_lo), core: 2. Of those that a mesh axis runs over, the one named last changes fastest.
Arguments:
- tokens: bfloat16 [32768, 7168], P(('ep', 'etp')), may hold values from -6 to 6
- expert_ids: int32 [32768, 8], P(('ep', 'etp')), may hold values from 0 to 383, all different within a row; in each aligned block of 128 rows (0 to 127, 128 to 255, ...) at most 3 rows name the same one
- gate_q: int32 [32768, 8], P(('ep', 'etp')), may hold values from 1 to 1024
- w_gate: bfloat16 [16, 7168, 2048], P('ep', None, 'etp'), may hold values from -0.0625 to 0.0625
- w_up: bfloat16 [16, 7168, 2048], P('ep', None, 'etp'), may hold values from -0.0625 to 0.0625
- w_down: bfloat16 [16, 2048, 7168], P('ep', 'etp'), may hold values from -0.125 to 0.125
Outputs:
- mixed: bfloat16 [32768, 7168], P(('ep', 'etp'))
The draws below stay inside these ranges and needn't reach their ends.
Inputs may be any that keep to these rules, and one draw needn't show every extreme that they name: `expert_ids`: each row names 8 different experts; among the 128 rows of one device no expert is named by more than 3 rows.
All inputs are finite; a program needn't handle non-finite values.
Results may differ from the reference program's by a relative error of at most 0.014.
Values may be sent and summed in bfloat16 or wider, within the bound.
No kernel may reach another device: no remote copies, remote signals or barrier semaphores. Data moves between devices by JAX's collectives and lax.ppermute only.
A program may use at most 64 MiB of HBM per device.

```python
import math
import jax
import jax.numpy as jnp
import numpy as np
from jax import lax

D = 7168
FF = 2048
EXPERTS_ALL = 384
TOP = 8
TOK_DEV = 128
CAP = 3
EXPERTS_WIN = 16
TOKENS = 32768
N_EP = 16
N_ETP = 16
DEVICES = 256


def plant(entries, stream_key, smallest, largest):
    place = [jax.random.randint(jax.random.fold_in(stream_key, axis), (), 0, length) for axis, length in enumerate(entries.shape)]
    main_axis = entries.shape.index(max(entries.shape))
    next_to = place[:main_axis] + [(place[main_axis] + 1) % entries.shape[main_axis]] + place[main_axis + 1:]
    return entries.at[tuple(place)].set(smallest).at[tuple(next_to)].set(largest)


def block_scale(own_key, extent, split, smallest, largest):
    def one(position, blocks):
        draws = jax.random.uniform(jax.random.fold_in(jax.random.fold_in(own_key, 6), position), (blocks,), jnp.float32, smallest / len(split), largest / len(split))
        return jnp.repeat(jnp.exp(draws), extent[position] // blocks).reshape((-1,) + (1,) * (len(extent) - position - 1))

    loudness = one(*split[0])
    for cut in split[1:]:
        loudness = loudness * one(*cut)
    return loudness


def deal_out(key, own, number, rows, number_of, top, limit, lean):
    sequence = jax.random.permutation(key, number_of)
    heavy_load, ordinary = portions_of(number_of, rows * top, limit, lean, True), portions_of(number_of, rows * top, limit, lean, False)
    places = jnp.arange(number_of)

    def named(sizes, offset_by):
        used = int((sizes > 0).sum())
        fixed = max(1, used // 4)
        shifted = fixed + (places - fixed + offset_by * (used - fixed)) % max(1, number_of - fixed)
        return jnp.zeros((number_of,), jnp.int32).at[sequence[jnp.where(places < fixed, places, shifted)]].set(jnp.asarray(sizes, jnp.int32))

    sizes = jnp.where(number % 4 == 0, named(heavy_load, number // 4), named(ordinary, number - number // 4 - 1))
    mixed = jax.random.permutation(jax.random.fold_in(own, 3), number_of)
    donor, receiver = mixed[0:number_of // 2 * 2:2], mixed[1:number_of // 2 * 2:2]
    room = jnp.minimum(sizes[donor] - 1, limit - sizes[receiver]) // 2
    room = jnp.where((donor == sequence[0]) | (receiver == sequence[0]) | (sizes[receiver] == 0), 0, jnp.maximum(room, 0))
    shifted = jax.random.randint(jax.random.fold_in(own, 4), (number_of // 2,), 0, 1 << 20) % (room + 1)
    sizes = sizes.at[donor].add(-shifted).at[receiver].add(shifted)
    items = jnp.searchsorted(jnp.cumsum(sizes), jnp.arange(rows * top), side="right").astype(jnp.int32)
    listing = items.reshape(top, rows).T
    listing = listing[jax.random.permutation(jax.random.fold_in(own, 1), rows)]
    offset_by = jax.random.randint(jax.random.fold_in(own, 2), (rows, 1), 0, top)
    return jnp.take_along_axis(listing, (jnp.arange(top)[None, :] + offset_by) % top, axis=1)


def portions_of(count, total, reach, lean, full):
    loads = [(1 << 20) // math.isqrt(standing ** lean) + 1 for standing in range(1, count + 1)]
    largest = reach if full else min(reach, max(-(-total // count), total * loads[0] // sum(loads)))
    least = 1 if total - largest >= count - 1 else 0
    holding, surplus = [largest] + [least] * (count - 1), total - largest - least * (count - 1)
    while surplus > 0:
        candidates = [i for i in range(1, count) if holding[i] < largest] or [i for i in range(1, count) if holding[i] < reach]
        mass, left = sum([loads[i] for i in candidates]), surplus
        for i in candidates:
            addition = min(reach - holding[i], max(1, left * loads[i] // mass), surplus)
            holding[i] = holding[i] + addition
            surplus = surplus - addition
    return np.array(holding)


def bell_draw(stream_key, shape, spread, reach, cuts=(), kind=jnp.bfloat16):
    values = jax.random.normal(stream_key, shape, jnp.float32) * spread
    if len(cuts) > 0:
        values = block_scale(stream_key, shape, cuts, -0.22, 0.18) * values
    return jnp.clip(values, min=-reach, max=reach).astype(kind)


def setup_inputs(seed: int = 0) -> dict:
    keys = jax.random.split(jax.random.key(seed), 7)
    tokens = bell_draw(keys[0], (TOKENS, D), 1.0, 6.0, ((0, 256),))
    expert_ids_keys = jax.random.split(jax.random.fold_in(keys[1], 1), TOKENS // TOK_DEV)
    expert_ids_turns = jax.random.permutation(jax.random.fold_in(keys[1], 3), TOKENS // TOK_DEV)
    expert_ids = jax.vmap(lambda own, number: deal_out(jax.random.fold_in(keys[1], 2), own, number, TOK_DEV, EXPERTS_ALL, TOP, CAP, 2))(expert_ids_keys, expert_ids_turns).reshape((TOKENS, TOP))
    gate_q = plant(jax.random.randint(keys[2], (TOKENS, TOP), 1, 1025), jax.random.fold_in(keys[2], 1), 1, 1024).astype(jnp.int32)
    w_gate = bell_draw(keys[3], (EXPERTS_WIN, D, FF), D ** -0.5, 0.0625, ((0, 16), (2, 16)))
    w_up = bell_draw(keys[4], (EXPERTS_WIN, D, FF), D ** -0.5, 0.0625, ((0, 16), (2, 16)))
    w_down = bell_draw(keys[5], (EXPERTS_WIN, FF, D), FF ** -0.5, 0.125, ((0, 16), (1, 16)))
    return dict(tokens=tokens, expert_ids=expert_ids, gate_q=gate_q, w_gate=w_gate, w_up=w_up, w_down=w_down)


def reference(tokens, expert_ids, gate_q, w_gate, w_up, w_down):
    slots = DEVICES * CAP
    group = FF // N_ETP
    weights = gate_q.astype(jnp.float32) / 1024.0

    def one_expert(carry, expert):
        match = expert_ids == expert
        token_weight = jnp.sum(jnp.where(match, weights, jnp.float32(0.0)), axis=1)
        used = jnp.any(match, axis=1)
        index = jnp.nonzero(used, size=slots, fill_value=0)[0].astype(jnp.int32)
        valid = jnp.arange(slots, dtype=jnp.int32) < jnp.sum(used.astype(jnp.int32))
        rows = tokens[index]
        gate = jnp.dot(rows, w_gate[expert], preferred_element_type=jnp.float32)
        upper = jnp.dot(rows, w_up[expert], preferred_element_type=jnp.float32)
        hidden = (jax.nn.silu(gate) * upper).astype(jnp.bfloat16)
        hidden_groups = hidden.reshape(slots, N_ETP, group).transpose(1, 0, 2)
        down_groups = w_down[expert].reshape(N_ETP, group, D)

        def add_group(total, pair):
            part = jnp.dot(pair[0], pair[1], preferred_element_type=jnp.float32).astype(jnp.bfloat16)
            return total + part.astype(jnp.float32), None

        summed, _ = lax.scan(add_group, jnp.zeros((slots, D), jnp.float32), (hidden_groups, down_groups))
        expert_out = summed.astype(jnp.bfloat16).astype(jnp.float32)
        scale = jnp.where(valid, token_weight[index], jnp.float32(0.0))
        carry = carry.at[index].add(scale[:, None] * expert_out)
        return carry, None

    total, _ = lax.scan(one_expert, jnp.zeros((TOKENS, D), jnp.float32), jnp.arange(N_EP, dtype=jnp.int32))
    return total.astype(jnp.bfloat16)
```

```python
import jax
import jax.numpy as jnp
from jax import lax
from jax.sharding import Mesh, PartitionSpec as P

CAP = 3
AX = ("y", "zl", "c", "zh", "x")
F32 = jnp.float32
BF16 = jnp.bfloat16


def shift(value, axis, step):
    n = lax.axis_size(axis)
    return lax.ppermute(value, axis, [(i, (i + step) % n) for i in range(n)])


def dot(a, b):
    return jnp.dot(a, b, preferred_element_type=F32)


def route(expert_ids, gate_q, groups):
    experts = jnp.arange(groups, dtype=jnp.int32)
    match = expert_ids[:, :, None] == experts[None, None, :]
    hot = jnp.sum(match.astype(F32), axis=1)
    gate = jnp.sum(jnp.where(match, gate_q[:, :, None].astype(F32), 0.0), axis=1) / 1024.0
    rows = expert_ids.shape[0]
    before = (jnp.arange(rows)[:, None] > jnp.arange(rows)[None, :]).astype(BF16)
    rank = dot(before, hot.astype(BF16))
    slot = jnp.arange(CAP, dtype=F32)
    chosen = (rank[:, :, None] == slot[None, None, :]) & (hot[:, :, None] > 0.0)
    placing = chosen.astype(BF16).reshape(rows, groups * CAP)
    scaling = jnp.where(chosen, gate[:, :, None], 0.0).reshape(rows, groups * CAP)
    return placing, scaling


def body(tokens, expert_ids, gate_q, w_gate, w_up, w_down):
    groups = lax.axis_size("y") * lax.axis_size("zl") * lax.axis_size("c")
    nx = lax.axis_size("x")
    width = tokens.shape[1]
    part = width // nx
    me = lax.axis_index("x")
    sources = groups * nx
    rows = sources * CAP
    half = rows // 2

    placing, scaling = route(expert_ids, gate_q, groups)
    bucket = jnp.einsum("tc,td->cd", placing, tokens, preferred_element_type=F32).astype(BF16)
    outgoing = bucket.reshape(groups, CAP, nx, part).transpose(0, 2, 1, 3)
    outgoing = outgoing.reshape(sources, 2, CAP * part // 2)
    arrived = lax.all_to_all(outgoing, ("y", "zl", "c", "x"), 0, 0, tiled=True)
    mine = arrived.reshape(rows, part)

    def slab(w, step, dim):
        start = ((me + step) % nx) * part
        return lax.dynamic_slice_in_dim(w, start, part, dim)

    both = [
        jnp.concatenate([slab(w_gate[0], k, 0), slab(w_up[0], k, 0)], axis=1) for k in range(nx)
    ]
    w_in = [both[0]] + [shift(both[k], "x", k) for k in range(1, nx)]
    down = [slab(w_down[0], k, 1) for k in range(nx)]
    w_out = [down[0]] + [shift(down[k], "x", k) for k in range(1, nx)]
    w_out = jnp.concatenate(w_out, axis=0)

    outs = []
    for c in range(2):
        own = mine[c * half : (c + 1) * half]
        quarter = half // 2
        up1 = shift(own, "zh", 1)
        dn1 = shift(own, "zh", -1)
        fa = shift(up1[:quarter], "zh", 1)
        fb = shift(dn1[quarter:], "zh", -1)
        x_all = jnp.concatenate([own, up1, dn1, fa, fb], axis=0)
        part_sum = [dot(x_all, w) for w in w_in]
        total = part_sum[0]
        for k in range(1, nx):
            total = total + shift(part_sum[k].astype(BF16), "x", -k).astype(F32)
        inner = total.shape[1] // 2
        hidden = (jax.nn.silu(total[:, :inner]) * total[:, inner:]).astype(BF16)
        pieces = [hidden] + [shift(hidden, "x", k) for k in range(1, nx)]
        term = dot(jnp.concatenate(pieces, axis=1), w_out)
        b0, bm, bp, b2 = jnp.split(term, 4, axis=0)
        ra = shift(b2[:quarter].astype(BF16), "zh", 1).astype(F32)
        rb = shift(b2[quarter:].astype(BF16), "zh", -1).astype(F32)
        sp1 = shift(bp[quarter:].astype(BF16), "zh", 1)
        sm1 = shift(bm[:quarter].astype(BF16), "zh", -1)
        sp2 = shift((bp[:quarter] + ra).astype(BF16), "zh", 1)
        sm2 = shift((bm[quarter:] + rb).astype(BF16), "zh", -1)
        from_m = jnp.concatenate([sp2, sp1], axis=0).astype(F32)
        from_p = jnp.concatenate([sm1, sm2], axis=0).astype(F32)
        outs.append((b0 + from_m + from_p).astype(BF16))
    local = jnp.concatenate(outs, axis=0)
    back = local.reshape(sources, 2, CAP * part // 2)
    results = lax.all_to_all(back, ("y", "zl", "c", "x"), 0, 0, tiled=True)
    flat = results.reshape(groups, nx, CAP, part).transpose(0, 2, 1, 3)
    flat = flat.reshape(groups * CAP, width)
    mixed = jnp.dot(scaling, flat.astype(F32))
    return mixed.astype(BF16)


def solution(mesh):
    devices = mesh.devices.reshape(4, 2, 2, 4, 4)
    fine = Mesh(devices, AX)
    ep, etp = ("y", "zl", "c"), ("zh", "x")
    in_specs = (
        P(AX, None),
        P(AX, None),
        P(AX, None),
        P(ep, None, etp),
        P(ep, etp, None),
    )
    in_specs = in_specs[:4] + (P(ep, None, etp), P(ep, etp, None))
    return jax.shard_map(body, mesh=fine, in_specs=in_specs, out_specs=P(AX, None), check_vma=False)
```

```python
import jax
import jax.numpy as jnp
from jax import lax
from jax.experimental import pallas as pl
from jax.experimental.pallas import tpu as pltpu
from jax.sharding import Mesh, PartitionSpec as P


CAP = 3
NX = 4
CHUNKS = 2
STEP = 256
AX = ("y", "zl", "c", "zh", "x")
F32 = jnp.float32
BF16 = jnp.bfloat16


def named(value, axis, step):
    n = lax.axis_size(axis)
    return lax.ppermute(value, axis, [(i, (i + step) % n) for i in range(n)])


def dot(a, b):
    return jnp.dot(a, b, preferred_element_type=F32)


def shape(*dims):
    return jax.ShapeDtypeStruct(dims, BF16)


def cost(flops, nbytes):
    return pl.CostEstimate(flops=flops, bytes_accessed=nbytes, transcendentals=0)


def route(expert_ids, gate_q, groups):
    experts = jnp.arange(groups, dtype=jnp.int32)
    match = expert_ids[:, :, None] == experts[None, None, :]
    hot = jnp.sum(match.astype(F32), axis=1)
    gate = jnp.sum(jnp.where(match, gate_q[:, :, None].astype(F32), 0.0), axis=1) / 1024.0
    rows = expert_ids.shape[0]
    before = (jnp.arange(rows)[:, None] > jnp.arange(rows)[None, :]).astype(BF16)
    rank = dot(before, hot.astype(BF16))
    slot = jnp.arange(CAP, dtype=F32)
    chosen = (rank[:, :, None] == slot[None, None, :]) & (hot[:, :, None] > 0.0)
    placing = chosen.astype(BF16).reshape(rows, groups * CAP)
    scaling = jnp.where(chosen, gate[:, :, None], 0.0).reshape(rows, groups * CAP)
    return placing, scaling


VMEM = pl.BlockSpec(memory_space=pltpu.VMEM)
SMEM = pl.BlockSpec(memory_space=pltpu.SMEM)
HBM = pl.BlockSpec(memory_space=pltpu.HBM)


def quarters(me, srcs, views, piece):

    def kernel(me_ref, *refs):
        n = len(srcs)
        ins, outs, held, sem_in, sem_out = refs[:n], refs[n : n + NX], refs[-3], refs[-2], refs[-1]
        loads, stores = [], []
        for k in (*range(1, NX), 0):
            at = lax.rem(me_ref[0] + k, NX)
            loads.append(
                [
                    pltpu.make_async_copy(views(ref, at), held.at[k, j], sem_in.at[k, j])
                    for j, ref in enumerate(ins)
                ]
            )
            stores.append(pltpu.make_async_copy(held.at[k], outs[k], sem_out.at[k]))
        for group in loads:
            for copy in group:
                copy.start()
        for group, store in zip(loads, stores):
            for copy in group:
                copy.wait()
            store.start()
        for store in stores:
            store.wait()

    n = len(srcs)
    return pl.pallas_call(
        kernel,
        out_shape=[shape(n, *piece)] * NX,
        in_specs=[SMEM] + [HBM] * n,
        out_specs=[HBM] * NX,
        scratch_shapes=[
            pltpu.VMEM((NX, n, *piece), BF16),
            pltpu.SemaphoreType.DMA((NX, n)),
            pltpu.SemaphoreType.DMA((NX,)),
        ],
        cost_estimate=cost(10**6, 4 * NX * n * piece[0] * piece[1]),
    )(me, *srcs)


def cut_in(me, w_gate, w_up):
    part = w_gate.shape[0] // NX

    def view(ref, at):
        return ref.at[pl.ds(pl.multiple_of(at * part, part), part)]

    return quarters(me, [w_gate, w_up], view, (part, w_gate.shape[1]))


def cut_out(me, w_down):
    part = w_down.shape[1] // NX

    def view(ref, at):
        return ref.at[:, pl.ds(pl.multiple_of(at * part, part), part)]

    outs = quarters(me, [w_down], view, (w_down.shape[0], part))
    return [out[0] for out in outs]


def gate_up(blocks, weights):
    _, part, cols = weights[0].shape
    rows = sum(b.shape[0] for b in blocks)
    nb = len(blocks)

    def kernel(*refs):
        xs, ws, outs = refs[:nb], refs[nb : nb + NX], refs[nb + NX :]
        x = jnp.concatenate([r[...] for r in xs], axis=0)
        for w, out in zip(ws, outs):
            pair = jnp.concatenate([w[0], w[1]], axis=1)
            out[...] = dot(x, pair).astype(BF16)

    return pl.pallas_call(
        kernel,
        out_shape=[shape(rows, 2 * cols)] * NX,
        in_specs=[VMEM] * (nb + NX),
        out_specs=[VMEM] * NX,
        cost_estimate=cost(4 * rows * part * cols * NX, 2 * part * (rows + 2 * cols * NX)),
        compiler_params=pltpu.CompilerParams(vmem_limit_bytes=16 * 2**20),
        name="gate_up",
    )(*blocks, *weights)


def project(pieces, weights, cuts):
    rows, cols = pieces[0].shape
    part = weights[0].shape[1]

    def kernel(*refs):
        hs, ws, outs = refs[:NX], refs[NX : 2 * NX], refs[2 * NX :]
        h = jnp.concatenate([r[...] for r in hs], axis=1)
        for at in range(0, part, STEP):
            w = jnp.concatenate([r[:, at : at + STEP] for r in ws], axis=0)
            term = dot(h, w).astype(BF16)
            top = 0
            for out, n in zip(outs, cuts):
                out[:, at : at + STEP] = term[top : top + n]
                top += n

    return pl.pallas_call(
        kernel,
        out_shape=[shape(n, part) for n in cuts],
        in_specs=[VMEM] * (2 * NX),
        out_specs=[VMEM] * len(cuts),
        cost_estimate=cost(2 * rows * part * cols * NX, 2 * part * (rows + cols * NX)),
        compiler_params=pltpu.CompilerParams(vmem_limit_bytes=24 * 2**20),
        name="project",
    )(*pieces, *weights)


def body(tokens, expert_ids, gate_q, w_gate, w_up, w_down):
    groups = lax.axis_size("y") * lax.axis_size("zl") * lax.axis_size("c")
    width = tokens.shape[1]
    part = width // NX
    me = lax.axis_index("x").astype(jnp.int32).reshape(1)
    sources = groups * NX
    rows = sources * CAP
    size = rows // CHUNKS
    w_gate, w_up, w_down = w_gate[0], w_up[0], w_down[0]

    placing, scaling = route(expert_ids, gate_q, groups)
    bucket = jnp.einsum("tc,td->cd", placing, tokens, preferred_element_type=F32)
    bucket = bucket.astype(BF16)
    outgoing = bucket.reshape(groups, CAP, NX, part).transpose(0, 2, 1, 3)
    outgoing = outgoing.reshape(sources, 2, CAP * part // 2)
    arrived = lax.all_to_all(outgoing, ("y", "zl", "c", "x"), 0, 0, tiled=True)
    mine = arrived.reshape(rows, part)

    wi, wo = cut_in(me, w_gate, w_up), cut_out(me, w_down)
    wi = [wi[0]] + [named(wi[k], "x", k) for k in range(1, NX)]
    wo = [wo[0]] + [named(wo[k], "x", k) for k in range(1, NX)]

    outs = []
    for c in range(CHUNKS):
        ahead = 1 - 2 * c
        own = mine[c * size : (c + 1) * size]
        up1 = named(own, "zh", 1)
        dn1 = named(own, "zh", -1)
        far = named(dn1 if c else up1, "zh", ahead)
        sums = gate_up([own, up1, dn1, far], wi)
        total = sums[0].astype(F32)
        for k in range(1, NX):
            total = total + named(sums[k], "x", -k).astype(F32)
        inner = total.shape[1] // 2
        hidden = (jax.nn.silu(total[:, :inner]) * total[:, inner:]).astype(BF16)
        pieces = [hidden] + [named(hidden, "x", k) for k in range(1, NX)]
        b0, bm, bp, b2 = project(pieces, wo, (size,) * 4)
        passed = named(b2, "zh", ahead).astype(F32)
        near = bm if c else bp
        near = (near.astype(F32) + passed).astype(BF16)
        from_m = named(bp if c else near, "zh", 1).astype(F32)
        from_p = named(near if c else bm, "zh", -1).astype(F32)
        outs.append((b0.astype(F32) + from_m + from_p).astype(BF16))
    local = jnp.concatenate(outs, axis=0)
    back = local.reshape(sources, 2, CAP * part // 2)
    results = lax.all_to_all(back, ("y", "zl", "c", "x"), 0, 0, tiled=True)
    flat = results.reshape(groups, NX, CAP, part).transpose(0, 2, 1, 3)
    flat = flat.reshape(groups * CAP, width)
    mixed = jnp.dot(scaling, flat.astype(F32))
    return mixed.astype(BF16)


def solution(mesh):
    fine = Mesh(mesh.devices.reshape(4, 2, 2, 4, 4), AX)
    ep, etp = ("y", "zl", "c"), ("zh", "x")
    rows = P(AX, None)
    in_specs = (rows, rows, rows, P(ep, None, etp), P(ep, None, etp), P(ep, etp, None))
    return jax.shard_map(body, mesh=fine, in_specs=in_specs, out_specs=rows, check_vma=False)
```
